32 devices in a mesh: seq: 16 (over z, x, core), head: 2 (over y).
Axes of the slice: x: 2, y: 2, z: 4, core: 2. Of those that a mesh axis runs over, the one named last changes fastest.
Arguments:
- query_rows: bfloat16 [8192, 64, 128], P('seq', 'head'), may hold values from -6 to 6
- key_rows: bfloat16 [8192, 64, 128], P('seq', 'head'), may hold values from -6 to 6
- value_rows: bfloat16 [8192, 64, 128], P('seq', 'head'), may hold values from -6 to 6
- log_decay: float32 [8192, 64], P('seq', 'head'), may hold values from -1.5 to 0, as said below
- state_in: float32 [128, 64, 128], P(None, 'head'), may hold values from -768 to 768
- decode_query: bfloat16 [8, 64, 128], P(None, 'head'), may hold values from -6 to 6
- decode_key: bfloat16 [8, 64, 128], P(None, 'head'), may hold values from -6 to 6
- decode_value: bfloat16 [8, 64, 128], P(None, 'head'), may hold values from -6 to 6
- decode_decay: float32 [8, 64], P(None, 'head'), may hold values from -0.5 to -0.02
Outputs:
- attended: bfloat16 [8192, 64, 128], P('seq', 'head')
- final_state: float32 [128, 64, 128], P('seq', 'head')
- decode_out: float32 [8, 64, 128], P(None, 'head')
The draws below stay inside these ranges and needn't reach their ends.
Inputs may be any that keep to these rules, and one draw needn't show every extreme that they name: log_decay is never positive.
All inputs are finite; a program needn't handle non-finite values.
Results may differ from the reference program's by a relative error of at most 0.0035.
Values sent between devices are 32-bit elements; how exact they have to be, the bound alone decides.
No kernel may reach another device: no remote copies, remote signals or barrier semaphores. Data moves between devices by JAX's collectives and lax.ppermute only.
A program may use at most 64 MiB of HBM per device.

```python
import jax
import jax.numpy as jnp
from jax import lax

HEAD_COUNT = 64
DH = 128
TOK_DEV = 512
GROUP = 512
DECODE = 8
WINDOW_TOKENS = 8192


def draw_log_decay(key, part):
    sequence_lanes = jax.random.split(key, 7)
    fast_cut = 5
    fast_heads = jax.random.randint(sequence_lanes[0], (HEAD_COUNT,), 0, 10) < fast_cut
    slow_total = jax.random.uniform(sequence_lanes[1], (HEAD_COUNT,), jnp.float32, 0.1, 0.5)
    fast_rate = jax.random.uniform(sequence_lanes[2], (HEAD_COUNT,), jnp.float32, 1.0 / 50.0, 1.0 / 30.0)
    baseline_decay_rate = jnp.where(fast_heads, fast_rate, slow_total / WINDOW_TOKENS)
    split_divisor = jax.random.uniform(sequence_lanes[3], (WINDOW_TOKENS // TOK_DEV, HEAD_COUNT), jnp.float32, 0.7, 1.4)
    split_divisor = jnp.repeat(split_divisor, TOK_DEV, axis=0)
    jitter_level = jax.random.uniform(sequence_lanes[4], (WINDOW_TOKENS, HEAD_COUNT), jnp.float32, 0.5, 1.5)
    spike_start_index = jax.random.randint(sequence_lanes[5], (2, HEAD_COUNT), 0, WINDOW_TOKENS)
    spike_length = jax.random.uniform(sequence_lanes[6], (2, HEAD_COUNT), jnp.float32, 0.22, 0.69)
    token_positions = jnp.arange(WINDOW_TOKENS)[:, None]
    decay_spikes = jnp.where(token_positions == spike_start_index[0][None, :], spike_length[0][None, :], 0.0)
    decay_spikes = decay_spikes + jnp.where(token_positions == spike_start_index[1][None, :], spike_length[1][None, :], 0.0)
    return -(baseline_decay_rate[None, :] * split_divisor * jitter_level + decay_spikes)


def level_of(own_key, dims, cuts, least, largest):
    def one(dim, parts):
        draws = jax.random.uniform(jax.random.fold_in(jax.random.fold_in(own_key, 6), dim), (parts,), jnp.float32, least / len(cuts), largest / len(cuts))
        return jnp.repeat(jnp.exp(draws), dims[dim] // parts).reshape((-1,) + (1,) * (len(dims) - dim - 1))

    gain = one(*cuts[0])
    for cut in cuts[1:]:
        gain = gain * one(*cut)
    return gain


def scatter_about(rng, dims, spread, most, shards=(), held_as=jnp.bfloat16):
    result = spread * jax.random.normal(rng, dims, jnp.float32)
    if shards:
        result = result * level_of(rng, dims, shards, -0.22, 0.18)
    return jnp.clip(result, -most, most).astype(held_as)


def setup_inputs(seed: int = 0) -> dict:
    key_of = jax.random.split(jax.random.key(seed), 10)
    return {
        "query_rows": scatter_about(key_of[0], (WINDOW_TOKENS, HEAD_COUNT, DH), 1.0, 6.0, ((0, 16), (1, 2))),
        "key_rows": scatter_about(key_of[1], (WINDOW_TOKENS, HEAD_COUNT, DH), 1.0, 6.0, ((0, 16), (1, 2))),
        "value_rows": scatter_about(key_of[2], (WINDOW_TOKENS, HEAD_COUNT, DH), 1.0, 6.0, ((0, 16), (1, 2))),
        "log_decay": draw_log_decay(jax.random.fold_in(key_of[9], 71), 0),
        "state_in": scatter_about(key_of[4], (DH, HEAD_COUNT, DH), 128.0, 768.0, ((1, 2),), jnp.float32),
        "decode_query": scatter_about(key_of[5], (DECODE, HEAD_COUNT, DH), 1.0, 6.0, ((1, 2),)),
        "decode_key": scatter_about(key_of[6], (DECODE, HEAD_COUNT, DH), 1.0, 6.0, ((1, 2),)),
        "decode_value": scatter_about(key_of[7], (DECODE, HEAD_COUNT, DH), 1.0, 6.0, ((1, 2),)),
        "decode_decay": jnp.clip(-0.5 + 0.48 * jax.random.uniform(key_of[8], (DECODE, HEAD_COUNT), jnp.float32) ** level_of(key_of[8], (DECODE, HEAD_COUNT), ((1, 2),), -0.2, 0.2), -0.5, -0.02),
    }


norm_eps = 1e-06

def normalize(mixed):
    return mixed * lax.rsqrt(lax.optimization_barrier(jnp.mean(mixed * mixed, axis=-1, keepdims=True)) + norm_eps)

def block_step(carried, pieces):
    queries, keys_blk, values_blk, decays = pieces
    cumulative = jnp.cumsum(decays, axis=0)
    transposed = cumulative.T
    token_positions = jnp.arange(GROUP)
    causal_mask = token_positions[:, None] >= token_positions[None, :]
    gaps = transposed[:, :, None] - transposed[:, None, :]
    factors = jnp.exp(jnp.where(causal_mask[None], gaps, -jnp.inf))
    query_wide = queries.astype(jnp.float32)
    key_wide = keys_blk.astype(jnp.float32)
    value_wide = values_blk.astype(jnp.float32)
    scores = jnp.einsum('ihd,jhd->hij', query_wide, key_wide, precision=lax.Precision.HIGHEST)
    masked = (scores * factors).astype(jnp.bfloat16).astype(jnp.float32)
    intra = jnp.einsum('hij,jhd->ihd', masked, value_wide, precision=lax.Precision.HIGHEST)
    inter = jnp.exp(cumulative)[:, :, None] * jnp.einsum('ihd,dhe->ihe', query_wide, carried, precision=lax.Precision.HIGHEST)
    attended = normalize(intra + inter).astype(jnp.bfloat16)
    last = cumulative[-1]
    weighted = key_wide * jnp.exp(last[None, :] - cumulative)[:, :, None]
    updated = jnp.exp(last)[None, :, None] * carried + jnp.einsum('jhd,jhe->dhe', weighted, value_wide, precision=lax.Precision.HIGHEST)
    return (updated, attended)

def reference(query_rows, key_rows, value_rows, log_decay, state_in, decode_query, decode_key, decode_value, decode_decay):
    blocks = WINDOW_TOKENS // GROUP
    shaped = (query_rows.reshape(blocks, GROUP, HEAD_COUNT, DH), key_rows.reshape(blocks, GROUP, HEAD_COUNT, DH), value_rows.reshape(blocks, GROUP, HEAD_COUNT, DH), log_decay.reshape(blocks, GROUP, HEAD_COUNT))
    final_state, outputs = lax.scan(block_step, state_in.astype(jnp.float32), shaped)
    attended = outputs.reshape(WINDOW_TOKENS, HEAD_COUNT, DH)
    running = final_state
    readings = []
    for step in range(DECODE):
        key_now = decode_key[step].astype(jnp.float32)
        value_now = decode_value[step].astype(jnp.float32)
        running = jnp.exp(decode_decay[step])[None, :, None] * running + key_now.T[:, :, None] * value_now[None, :, :]
        query_now = decode_query[step].astype(jnp.float32)
        readings.append(jnp.einsum('hd,dhe->he', query_now, running, precision=lax.Precision.HIGHEST))
    decode_out = normalize(jnp.stack(readings, axis=0))
    return (attended, final_state, decode_out)
```

```python
import functools

import jax
import jax.numpy as jnp
from jax import lax
from jax.experimental import pallas as pl
from jax.experimental.pallas import tpu as pltpu
from jax.sharding import PartitionSpec as P

norm_eps = 1e-06
LANES = 128
SUB = 8
HIGH = lax.Precision.HIGHEST
F32 = jnp.float32
BF16 = jnp.bfloat16


def split3(x):
    hi = x.astype(BF16)
    rest = x - hi.astype(F32)
    mid = rest.astype(BF16)
    low = (rest - mid.astype(F32)).astype(BF16)
    return hi, mid, low


def split2(x):
    hi = x.astype(BF16)
    return hi, (x - hi.astype(F32)).astype(BF16)


def triangle_sum(rows, keep):
    tokens = rows.shape[1]
    s = lax.broadcasted_iota(jnp.int32, (tokens, tokens), 0)
    t = lax.broadcasted_iota(jnp.int32, (tokens, tokens), 1)
    ones = jnp.where(keep(s, t), 1.0, 0.0).astype(BF16)
    total = None
    for piece in split3(rows):
        part = jnp.dot(piece, ones, preferred_element_type=F32)
        total = part if total is None else total + part
    return total


def columns_of(rows):
    return jnp.transpose(rows, (1, 0))


def by_head(ref, scratch):
    tokens, heads, width = ref.shape
    scratch[...] = ref[...].astype(F32).reshape(tokens * heads, width)


def head_rows(scratch, head):
    return scratch[pl.ds(head, scratch.shape[0] // SUB, stride=SUB), :]


def state_kernel(tiled, pseudo, rows, ld_ref, k_ref, v_ref, qd_ref, pos_ref, *refs):
    if tiled:
        keep_ref, send_ref, tot_ref, kf, vf = refs
    else:
        state_ref, tot_ref, kf, vf = refs
    group = pl.program_id(0)
    decays = ld_ref[...]
    tot_ref[...] = jnp.broadcast_to(jnp.sum(decays, axis=1, keepdims=True), (SUB, LANES))
    to_end = columns_of(jnp.exp(triangle_sum(decays, lambda s, t: s > t)))
    by_head(k_ref, kf)
    by_head(v_ref, vf)
    if tiled:
        core, xbit = pos_ref[0] == 1, pos_ref[1] == 1

    def place(slot, square):
        spans = square.shape[0] // (4 * rows)
        for z in range(spans):
            piece = [square[(z * 4 + i) * rows : (z * 4 + i + 1) * rows] for i in range(4)]
            for x_rel in range(2):
                def pick(c_rel):
                    near = jnp.where(core, piece[2 * x_rel + 1 - c_rel], piece[2 * x_rel + c_rel])
                    far = jnp.where(core, piece[2 * (1 - x_rel) + 1 - c_rel], piece[2 * (1 - x_rel) + c_rel])
                    return jnp.where(xbit, far, near)
                keep_ref[x_rel, z, slot] = pick(0)
                send_ref[x_rel, z, slot] = pick(1)

    readings = []
    for i in range(SUB):
        keys = head_rows(kf, i).astype(BF16)
        weighted = head_rows(vf, i) * to_end[:, i : i + 1]
        hi, low = split2(weighted)
        both = lax.dot_general(keys, jnp.concatenate([hi, low], axis=1), (((0,), (0,)), ((), ())), preferred_element_type=F32)
        state = both[:, :LANES] + both[:, LANES:]
        if pseudo:
            hi, low = split2(state)
            read = jnp.dot(qd_ref[i], jnp.concatenate([hi, low], axis=1), preferred_element_type=F32)
            readings.append(read[:, :LANES] + read[:, LANES:])
        if tiled:
            place(group * SUB + i, state)
        else:
            state_ref[i] = state
    if pseudo:
        slot = keep_ref.shape[2] - 1
        half = SUB // 4
        for zz in range(half):
            piece = readings[4 * zz : 4 * zz + 4]
            for x_rel in range(2):
                def pick(c_rel):
                    near = jnp.where(core, piece[2 * x_rel + 1 - c_rel], piece[2 * x_rel + c_rel])
                    far = jnp.where(core, piece[2 * (1 - x_rel) + 1 - c_rel], piece[2 * (1 - x_rel) + c_rel])
                    return jnp.where(xbit, far, near)
                keep_ref[x_rel, group * half + zz, slot] = pick(0)
                send_ref[x_rel, group * half + zz, slot] = pick(1)


def states(chunk, heads, tiled, pseudo, rows, spans, pos, decays, key_rows, value_rows, dec_query):
    tokens, _, width = key_rows.shape
    groups = heads // SUB
    first = chunk * groups
    slots = heads + (1 if pseudo else 0)
    block = pl.BlockSpec((tokens, SUB, width), lambda g: (0, first + g, 0))
    tot = jax.ShapeDtypeStruct((heads, LANES), F32)
    tot_spec = pl.BlockSpec((SUB, LANES), lambda g: (g, 0))
    if tiled:
        shape = jax.ShapeDtypeStruct((2, spans, slots, rows, width), F32)
        whole = pl.BlockSpec((2, spans, slots, rows, width), lambda g: (0, 0, 0, 0, 0))
        out_shape, out_specs = (shape, shape, tot), (whole, whole, tot_spec)
    else:
        out_shape = (jax.ShapeDtypeStruct((heads, width, width), F32), tot)
        out_specs = (pl.BlockSpec((SUB, width, width), lambda g: (g, 0, 0)), tot_spec)
    return pl.pallas_call(
        functools.partial(state_kernel, tiled, pseudo, rows),
        grid=(groups,),
        in_specs=[
            pl.BlockSpec((SUB, tokens), lambda g: (first + g, 0)),
            block,
            block,
            pl.BlockSpec((SUB,) + dec_query.shape[1:], lambda g: (first + g, 0, 0)),
            pl.BlockSpec(memory_space=pltpu.SMEM),
        ],
        out_specs=out_specs,
        out_shape=out_shape,
        scratch_shapes=[pltpu.VMEM((tokens * SUB, width), F32)] * 2,
        cost_estimate=pl.CostEstimate(flops=4 * heads * tokens * width * width, transcendentals=heads * tokens, bytes_accessed=4 * heads * tokens * width),
        name="states",
    )(decays, key_rows, value_rows, dec_query, pos)


def intra_kernel(tile, ld_ref, q_ref, k_ref, v_ref, intra_ref, qh_ref, qf, kf, vf):
    tokens = q_ref.shape[0]
    cum = triangle_sum(ld_ref[...], lambda s, t: s <= t)
    cols = columns_of(cum)
    by_head(q_ref, qf)
    by_head(k_ref, kf)
    by_head(v_ref, vf)
    row = lax.broadcasted_iota(jnp.int32, (tile, tile), 0)
    col = lax.broadcasted_iota(jnp.int32, (tile, tile), 1)
    causal = row >= col
    for i in range(SUB):
        queries = head_rows(qf, i).astype(BF16)
        keys = head_rows(kf, i).astype(BF16)
        values = head_rows(vf, i).astype(BF16)
        qh_ref[i] = queries
        for start in range(0, tokens, tile):
            end = start + tile
            scores = lax.dot_general(queries[start:end], keys[:end], (((1,), (1,)), ((), ())), preferred_element_type=F32)
            gaps = cols[start:end, i : i + 1] - cum[i : i + 1, :end]
            inside = jnp.where(causal, gaps[:, start:], -jnp.inf)
            if start:
                gaps = jnp.concatenate([gaps[:, :start], inside], axis=1)
            else:
                gaps = inside
            masked = (scores * jnp.exp(gaps)).astype(BF16)
            intra_ref[i, start:end] = jnp.dot(masked, values[:end], preferred_element_type=F32)


def inside_blocks(group, count, decays, query_rows, key_rows, value_rows):
    tokens, _, width = query_rows.shape
    block = pl.BlockSpec((tokens, SUB, width), lambda g: (0, group + g, 0))
    out = pl.BlockSpec((SUB, tokens, width), lambda g: (g, 0, 0))
    return pl.pallas_call(
        functools.partial(intra_kernel, 128),
        grid=(count,),
        in_specs=[pl.BlockSpec((SUB, tokens), lambda g: (group + g, 0)), block, block, block],
        out_specs=(out, out),
        out_shape=(
            jax.ShapeDtypeStruct((count * SUB, tokens, width), F32),
            jax.ShapeDtypeStruct((count * SUB, tokens, width), BF16),
        ),
        scratch_shapes=[pltpu.VMEM((tokens * SUB, width), F32)] * 3,
        cost_estimate=pl.CostEstimate(flops=4 * count * SUB * tokens * tokens * width, transcendentals=count * SUB * tokens * tokens, bytes_accessed=12 * count * SUB * tokens * width),
        name="inside",
    )(decays, query_rows, key_rows, value_rows)


def output_kernel(tiled, ld_ref, qh_ref, intra_ref, *refs):
    if tiled:
        near_ref, far_ref, pos_ref, out_ref, flat = refs
        core, xbit = pos_ref[0] == 1, pos_ref[1] == 1
    else:
        state_ref, out_ref, flat = refs
    tokens = out_ref.shape[0]
    cols = columns_of(jnp.exp(triangle_sum(ld_ref[...], lambda s, t: s <= t)))
    for i in range(SUB):
        if tiled:
            pieces = []
            for z in range(near_ref.shape[1]):
                for x in range(2):
                    for c in range(2):
                        first = near_ref if c == 0 else far_ref
                        second = far_ref if c == 0 else near_ref
                        plain = jnp.where(core, second[x, z, i], first[x, z, i])
                        flipped = jnp.where(core, second[1 - x, z, i], first[1 - x, z, i])
                        pieces.append(jnp.where(xbit, flipped, plain))
            carried = jnp.concatenate(pieces, axis=0)
        else:
            carried = state_ref[i]
        hi, low = split2(carried)
        both = jnp.dot(qh_ref[i], jnp.concatenate([hi, low], axis=1), preferred_element_type=F32)
        mixed = intra_ref[i] + cols[:, i : i + 1] * (both[:, :LANES] + both[:, LANES:])
        mean = jnp.mean(mixed * mixed, axis=1, keepdims=True)
        flat[pl.ds(i, tokens, stride=SUB), :] = mixed * lax.rsqrt(mean + norm_eps)
    out_ref[...] = flat[...].reshape(out_ref.shape).astype(BF16)


def outputs(tiled, heads, chunk, decays, qh, intra, pos, *carried):
    tokens, width = qh.shape[1:]
    groups = heads // SUB
    first = chunk * groups
    block = pl.BlockSpec((SUB, tokens, width), lambda g: (g, 0, 0))
    if tiled:
        _, spans, _, rows, _ = carried[0].shape
        part = pl.BlockSpec((2, spans, SUB, rows, width), lambda g: (0, 0, g, 0, 0))
        specs = [part, part, pl.BlockSpec(memory_space=pltpu.SMEM)]
        extra = carried + (pos,)
    else:
        specs = [pl.BlockSpec((SUB, width, width), lambda g: (g, 0, 0))]
        extra = carried
    return pl.pallas_call(
        functools.partial(output_kernel, tiled),
        grid=(groups,),
        in_specs=[pl.BlockSpec((SUB, tokens), lambda g: (first + g, 0)), block, block] + specs,
        out_specs=pl.BlockSpec((tokens, SUB, width), lambda g: (0, g, 0)),
        out_shape=jax.ShapeDtypeStruct((tokens, heads, width), BF16),
        scratch_shapes=[pltpu.VMEM((tokens * SUB, width), F32)],
        cost_estimate=pl.CostEstimate(flops=4 * heads * tokens * width * width, transcendentals=2 * heads * tokens, bytes_accessed=8 * heads * tokens * width),
        name="outputs",
    )(decays, qh, intra, *extra)


def decode_matrix(decay):
    steps = decay.shape[0]
    cum = jnp.cumsum(decay, axis=0)
    order = jnp.arange(steps)
    causal = (order[:, None] >= order[None, :]).reshape((steps, steps) + (1,) * (decay.ndim - 1))
    return jnp.exp(jnp.where(causal, cum[:, None] - cum[None, :], -jnp.inf)), jnp.exp(cum)


def normalize(mixed):
    return mixed * lax.rsqrt(jnp.mean(mixed * mixed, axis=-1, keepdims=True) + norm_eps)


def local(query_rows, key_rows, value_rows, log_decay, state_in, decode_query, decode_key, decode_value, decode_decay):
    tokens, heads, width = query_rows.shape
    steps = decode_query.shape[0]
    n = lax.axis_size("seq")
    me = lax.axis_index("seq")
    spans = n // 4
    rows = width // n
    core, xbit, z = me % 2, (me // 2) % 2, me // 4
    tiled = rows % SUB == 0
    pseudo = tiled and rows == steps and heads % n == 0 and n % SUB == 0 and n * steps == width
    chunks = heads // n if pseudo else 1
    per = heads // chunks
    slots = per + (1 if pseudo else 0)
    pos = jnp.stack([core, xbit]).astype(jnp.int32)
    decays = jnp.transpose(log_decay)
    dec_query = jnp.transpose(decode_query, (1, 0, 2))

    swap_core = [(i, i ^ 1) for i in range(n)]
    swap_x = [(i, i ^ 2) for i in range(n)]
    shift = lambda s: [(i, (i + 4 * s) % n) for i in range(n)]

    def first(flag, a, b):
        return jnp.where(flag == 0, a, b)

    def weights(total, part):
        w = jnp.exp(total)[:, None, :]
        if pseudo:
            lead = part.shape[:-1]
            w = jnp.broadcast_to(w, lead + w.shape)
            w = jnp.concatenate([w, jnp.exp(part)[..., None, None, :]], axis=len(lead))
        return w

    def owners(total, x_rel):
        if not pseudo:
            return None
        t = total.reshape(spans, 2, 2, LANES)
        t = lax.dynamic_index_in_dim(t, core, 2, keepdims=False)
        return lax.dynamic_index_in_dim(t, (xbit + x_rel) % 2, 1, keepdims=False)

    def exchange(x, total, pairs):
        flat = jnp.concatenate([x.reshape(-1, width), total], axis=0)
        got = lax.ppermute(flat, "seq", pairs)
        return got[: -total.shape[0]].reshape(x.shape), got[-total.shape[0] :]

    def to_absolute(pieces):
        turned = jnp.stack(pieces[::-1] + pieces[:0:-1])
        return lax.dynamic_slice_in_dim(turned, spans - 1 - z, spans, 0)

    if pseudo:
        def own_head(x, axis, c):
            return lax.dynamic_index_in_dim(x, c * n + me, axis, keepdims=False)

        dec_terms = []
        for c in range(chunks):
            q, k, v, d = (own_head(a, 1, c).astype(F32) for a in (decode_query, decode_key, decode_value, decode_decay))
            pair, from_end = decode_matrix(d)
            near = jnp.dot(jnp.dot(q, k.T, precision=HIGH) * pair, v, precision=HIGH)
            before = jnp.dot(q, own_head(state_in, 1, c), precision=HIGH)
            dec_terms.append((from_end[:, None], near, before))
    prior = jnp.transpose(lax.dynamic_slice_in_dim(state_in, me * rows, rows, 0), (1, 0, 2))

    kept = []
    for c in range(chunks):
        made = states(c, per, tiled, pseudo, rows, spans, pos, decays, key_rows, value_rows, dec_query)
        if tiled:
            keep, send, total = made
        else:
            whole, total = made
            parts = jnp.transpose(whole.reshape(per, spans, 2, 2, rows, width), (3, 2, 1, 0, 4, 5))
            parts = jnp.where(xbit == 0, parts, parts[:, ::-1])
            keep, send = first(core, parts[0], parts[1]), first(core, parts[1], parts[0])
        kept.append((keep, send, total))

    groups = heads // SUB
    insides = [inside_blocks(c * (groups // chunks), groups // chunks, decays, query_rows, key_rows, value_rows) for c in range(chunks)]

    level = []
    for c in range(chunks):
        keep, send, total = kept[c]
        got, got_total = exchange(send, total, swap_core)
        part = lambda t: jnp.stack([owners(t, 0), owners(t, 1)]) if pseudo else None
        mine = first(core, weights(got_total, part(got_total)), 1.0)
        theirs = first(core, 1.0, weights(total, part(total)))
        chip = keep * mine + got * theirs
        chip_total = total + got_total
        got_x, got_x_total = exchange(chip[1], chip_total, swap_x)
        mine = first(xbit, weights(got_x_total, owners(got_x_total, 0)), 1.0)
        theirs = first(xbit, 1.0, weights(chip_total, owners(chip_total, 0)))
        span = chip[0] * mine + got_x * theirs
        level.append((got, got_total, chip, chip_total, got_x, got_x_total, span, chip_total + got_x_total))

    finals, decoded, carries = [], [], []
    for c in range(chunks):
        span, span_total = level[c][6:]
        pieces = [lax.dynamic_index_in_dim(span, z, 0, keepdims=False)]
        totals = [span_total]
        for s in range(1, spans):
            piece, t = exchange(lax.dynamic_index_in_dim(span, (z + s) % spans, 0, keepdims=False), span_total, shift(s))
            pieces.append(piece)
            totals.append(t)
        pieces, totals = to_absolute(pieces), to_absolute(totals)
        carried = prior[c * per : (c + 1) * per]
        if pseudo:
            carried = jnp.concatenate([carried, dec_terms[c][2][None]], axis=0)
        all_carried = []
        for s in range(spans):
            all_carried.append(carried)
            t = totals[s]
            own = lax.dynamic_index_in_dim(t, me, 0, keepdims=False) if pseudo else None
            carried = carried * weights(t, own) + pieces[s]
        finals.append(carried[:per])
        if pseudo:
            from_end, near, _ = dec_terms[c]
            dec = normalize(carried[per] * from_end + near)
            all_carried = [jnp.concatenate([a[:per], dec[None]], axis=0) for a in all_carried]
        all_carried = jnp.stack(all_carried)
        pieces = [lax.dynamic_index_in_dim(all_carried, z, 0, keepdims=False)]
        for s in range(1, spans):
            pieces.append(lax.ppermute(lax.dynamic_index_in_dim(all_carried, (z + s) % spans, 0, keepdims=False), "seq", shift(s)))
        carries.append(to_absolute(pieces))

    def advance(carried, total, state):
        new = carried[..., :per, :, :] * jnp.exp(total)[:, None, :] + state[..., :per, :, :]
        return jnp.concatenate([new, carried[..., per:, :, :]], axis=-3) if pseudo else new

    attended, dec_out = [], []
    for c in range(chunks):
        keep, send, total = kept[c]
        got, got_total, chip, chip_total, got_x, got_x_total, _, _ = level[c]
        at_span = carries[c]
        msg = first(xbit, advance(at_span, chip_total, chip[0]), at_span)
        own = first(xbit, at_span, advance(at_span, got_x_total, got_x))
        at_chip = jnp.stack([own, lax.ppermute(msg, "seq", swap_x)])
        msg = first(core, advance(at_chip, total, keep), at_chip)
        own = first(core, at_chip, advance(at_chip, got_total, got))
        other = lax.ppermute(msg, "seq", swap_core)
        intra, qh = insides[c]
        if tiled:
            carried = (own, other)
        else:
            both = jnp.stack([first(core, own, other), first(core, other, own)])
            both = jnp.where(xbit == 0, both, both[:, ::-1])
            carried = (jnp.transpose(both, (3, 2, 1, 0, 4, 5)).reshape(per, width, width),)
        attended.append(outputs(tiled, per, c, decays, qh, intra, pos, *carried))
        if pseudo:
            both = jnp.stack([first(core, own[:, :, per], other[:, :, per]), first(core, other[:, :, per], own[:, :, per])])
            both = jnp.where(xbit == 0, both, both[:, ::-1])
            dec_out.append(jnp.transpose(both, (3, 2, 1, 0, 4)).reshape(steps, per, width))

    attended = jnp.concatenate(attended, axis=1)
    final_rows = jnp.transpose(jnp.concatenate(finals, axis=0), (1, 0, 2))
    if pseudo:
        decode_out = jnp.concatenate(dec_out, axis=1)
    else:
        start = me * rows
        key_part = lax.dynamic_slice_in_dim(decode_key, start, rows, 2).astype(F32)
        query_part = lax.dynamic_slice_in_dim(decode_query, start, rows, 2).astype(F32)
        pair, from_end = decode_matrix(decode_decay)
        scores = jnp.einsum("thr,shr->tsh", query_part, key_part, precision=HIGH) * pair
        near = jnp.einsum("tsh,she->the", scores, decode_value.astype(F32), precision=HIGH)
        far = jnp.einsum("thr,rhe->the", query_part, final_rows, precision=HIGH) * from_end[:, :, None]
        decode_out = normalize(lax.psum(near + far, "seq"))
    return attended, final_rows, decode_out


def solution(mesh):
    in_specs = (
        P("seq", "head", None),
        P("seq", "head", None),
        P("seq", "head", None),
        P("seq", "head"),
        P(None, "head", None),
        P(None, "head", None),
        P(None, "head", None),
        P(None, "head", None),
        P(None, "head"),
    )
    out_specs = (P("seq", "head", None), P("seq", "head", None), P(None, "head", None))
    return jax.shard_map(local, mesh=mesh, in_specs=in_specs, out_specs=out_specs, check_vma=False)
```

```python
import functools

import jax
import jax.numpy as jnp
from jax import lax
from jax.experimental import pallas as pl
from jax.experimental.pallas import tpu as pltpu
from jax.sharding import PartitionSpec as P

norm_eps = 1e-06
LANES = 128
SUB = 8
F32 = jnp.float32
BF16 = jnp.bfloat16
HIGH = lax.Precision.HIGHEST
VM = pl.BlockSpec(memory_space=pltpu.VMEM)
HBM = pl.BlockSpec(memory_space=pltpu.MemorySpace.HBM)
MIB = 1 << 20


def split3(x):
    hi = x.astype(BF16)
    rest = x - hi.astype(F32)
    mid = rest.astype(BF16)
    low = (rest - mid.astype(F32)).astype(BF16)
    return hi, mid, low


def split2(x):
    hi = x.astype(BF16)
    return hi, (x - hi.astype(F32)).astype(BF16)


def exact_dot(x, ones, dims):
    total = None
    for piece in split3(x):
        part = lax.dot_general(piece, ones, (dims, ((), ())), preferred_element_type=F32)
        total = part if total is None else total + part
    return total


def triangle_sum(decays, keep):
    tokens = decays.shape[0]
    s = lax.broadcasted_iota(jnp.int32, (tokens, tokens), 0)
    t = lax.broadcasted_iota(jnp.int32, (tokens, tokens), 1)
    ones = jnp.where(keep(s, t), 1.0, 0.0).astype(BF16)
    return exact_dot(decays, ones, ((0,), (0,)))


def flatten(block, scratch):
    tokens, heads, width = block.shape
    scratch[...] = block.astype(F32).reshape(tokens * heads, width)


def head_rows(scratch, head, heads):
    return scratch[pl.ds(head, scratch.shape[0] // heads, stride=heads), :]


def position():
    me = lax.axis_index("seq")
    return lax.rem(me, 2) == 1, lax.rem(lax.div(me, 2), 2) == 1


def one_group(tiled, pseudo, rows, slot0, group, decay_col, k_block, v_block, dq, head0, kf, vf, outs):
    keep_ref, send_ref, kh_ref, vh_ref = outs
    flatten(k_block, kf)
    flatten(v_block, vf)
    if tiled:
        core, xbit = position()
        spans, slots = keep_ref.shape[1:3]

    def place(slot, z, piece):
        for x_rel in range(2):
            for c_rel in range(2):
                near = jnp.where(core, piece[2 * x_rel + 1 - c_rel], piece[2 * x_rel + c_rel])
                far = jnp.where(core, piece[2 * (1 - x_rel) + 1 - c_rel], piece[2 * (1 - x_rel) + c_rel])
                tile = jnp.where(xbit, far, near)
                if c_rel == 0:
                    keep_ref[x_rel, z, slot] = tile
                else:
                    start = ((x_rel * spans + z) * slots + slot) * rows
                    send_ref[start : start + rows] = tile

    readings = []
    for i in range(SUB):
        keys = head_rows(kf, i, SUB).astype(BF16)
        values = head_rows(vf, i, SUB)
        kh_ref[slot0 + i] = keys
        vh_ref[slot0 + i] = values.astype(BF16)
        hi, low = split2(values * decay_col(i))
        both = lax.dot_general(keys, jnp.concatenate([hi, low], axis=1), (((0,), (0,)), ((), ())), preferred_element_type=F32)
        state = both[:, :LANES] + both[:, LANES:]
        if pseudo:
            hi, low = split2(state)
            query = head_rows(dq, head0 + i, dq.shape[0] // SUB).astype(BF16)
            read = jnp.dot(query, jnp.concatenate([hi, low], axis=1), preferred_element_type=F32)
            readings.append(read[:, :LANES] + read[:, LANES:])
        if tiled:
            for z in range(spans):
                place(slot0 + i, z, [state[(z * 4 + j) * rows : (z * 4 + j + 1) * rows] for j in range(4)])
        else:
            keep_ref[slot0 + i] = state
    for j in range(0, len(readings), 4):
        place(slots - 1, (slot0 + j) // 4, readings[j : j + 4])


def state_kernel(tiled, pseudo, rows, per, lead, *refs):
    tokens = lead[0]
    groups = per // SUB
    first = lead[1] == 0
    heads = lead[2]
    rest = heads - per
    if first:
        refs = list(refs)
        ld_ref, dq_ref, k_hbm, v_hbm = refs[:4]
        keep_ref, send_ref, tot_ref, kh_ref, vh_ref = refs[4:9]
        at = 9
        if rest:
            wcol_ref, tall_ref, krest_ref, vrest_ref = refs[9:13]
            at = 13
        kf, vf, dq, kbuf, vbuf, sems = refs[at:]
        copies = []
        for g in range(groups):
            span = pl.ds(g * SUB, SUB)
            copies.append((
                pltpu.make_async_copy(k_hbm.at[:, span, :], kbuf.at[g], sems.at[2 * g]),
                pltpu.make_async_copy(v_hbm.at[:, span, :], vbuf.at[g], sems.at[2 * g + 1]),
            ))
        if rest:
            span = pl.ds(per, rest)
            copies.append((
                pltpu.make_async_copy(k_hbm.at[:, span, :], krest_ref, sems.at[2 * groups]),
                pltpu.make_async_copy(v_hbm.at[:, span, :], vrest_ref, sems.at[2 * groups + 1]),
            ))
        for pair in copies:
            for copy in pair:
                copy.start()
        decays = ld_ref[...]
        wcol = jnp.transpose(jnp.exp(triangle_sum(decays, lambda s, t: s > t)), (1, 0))
        tall = exact_dot(decays, jnp.ones((tokens, LANES), BF16), ((0,), (0,)))
        totals = tall[:per]
        if rest:
            wcol_ref[...] = wcol
            tall_ref[...] = tall
        head0 = 0
    else:
        wcol_ref, tall_ref, dq_ref, krest_ref, vrest_ref, keep_ref, send_ref, tot_ref, kh_ref, vh_ref, kf, vf, dq = refs
        head0 = lead[1]
        wcol = wcol_ref[...]
        totals = tall_ref[head0 : head0 + per]
    tot_ref[...] = totals
    if tiled:
        send_ref[send_ref.shape[0] - per :] = totals
    if pseudo:
        flatten(dq_ref[...], dq)
    for g in range(groups):
        if first:
            for copy in copies[g]:
                copy.wait()
            k_block, v_block = kbuf[g], vbuf[g]
        else:
            at = head0 - (heads - krest_ref.shape[1]) + g * SUB
            k_block, v_block = krest_ref[:, at : at + SUB, :], vrest_ref[:, at : at + SUB, :]
        base = head0 + g * SUB
        one_group(tiled, pseudo, rows, g * SUB, g, lambda i: wcol[:, base + i : base + i + 1], k_block, v_block, dq, base, kf, vf, (keep_ref, send_ref, kh_ref, vh_ref))
    if first and rest:
        for copy in copies[-1]:
            copy.wait()


def states(chunk, per, tiled, pseudo, rows, spans, arrays):
    first = chunk == 0
    if first:
        log_decay, dec_query, key_rows, value_rows = arrays
        tokens, heads, width = key_rows.shape
    else:
        wcol, tall, dec_query, krest, vrest = arrays
        tokens, heads = wcol.shape
        width = krest.shape[2]
    rest = heads - per
    slots = per + (1 if pseudo else 0)
    if tiled:
        keep = jax.ShapeDtypeStruct((2, spans, slots, rows, width), F32)
        send = jax.ShapeDtypeStruct((2 * spans * slots * rows + per, width), F32)
    else:
        keep = jax.ShapeDtypeStruct((per, width, width), F32)
        send = jax.ShapeDtypeStruct((SUB, width), F32)
    by_head = jax.ShapeDtypeStruct((per, tokens, width), BF16)
    out_shape = [keep, send, jax.ShapeDtypeStruct((per, width), F32), by_head, by_head]
    scratch = [
        pltpu.VMEM((tokens * SUB, width), F32),
        pltpu.VMEM((tokens * SUB, width), F32),
        pltpu.VMEM((dec_query.shape[0] * heads, width), F32),
    ]
    if first:
        if rest:
            out_shape += [jax.ShapeDtypeStruct((tokens, heads), F32), jax.ShapeDtypeStruct((heads, width), F32)]
            out_shape += [jax.ShapeDtypeStruct((tokens, rest, width), BF16)] * 2
        scratch += [pltpu.VMEM((per // SUB, tokens, SUB, width), BF16)] * 2
        scratch += [pltpu.SemaphoreType.DMA((2 * (per // SUB) + 2,))]
        in_specs = [VM, VM, HBM, HBM]
    else:
        in_specs = [VM] * 5
    return pl.pallas_call(
        functools.partial(state_kernel, tiled, pseudo, rows, per, (tokens, chunk * per, heads)),
        in_specs=in_specs,
        out_specs=[VM] * len(out_shape),
        out_shape=out_shape,
        scratch_shapes=scratch,
        cost_estimate=pl.CostEstimate(flops=4 * per * tokens * width * width, transcendentals=per * tokens, bytes_accessed=4 * per * tokens * width),
        compiler_params=pltpu.CompilerParams(vmem_limit_bytes=LIMITS["states"] * MIB),
        name="states",
    )(*arrays)


def inside_kernel(tile, head0, slot0, ld_ref, q_ref, kh_ref, vh_ref, intra_ref, q2_ref, qf):
    tokens = q_ref.shape[0]
    cum = triangle_sum(ld_ref[:, head0 : head0 + SUB], lambda s, t: s <= t)
    cols = jnp.transpose(cum, (1, 0))
    grown = jnp.exp(cols)
    flatten(q_ref[:, head0 : head0 + SUB, :], qf)
    row = lax.broadcasted_iota(jnp.int32, (tile, tile), 0)
    col = lax.broadcasted_iota(jnp.int32, (tile, tile), 1)
    causal = row >= col
    for i in range(SUB):
        wide = head_rows(qf, i, SUB)
        queries = wide.astype(BF16)
        hi, low = split2(wide * grown[:, i : i + 1])
        q2_ref[i, :, :LANES] = hi
        q2_ref[i, :, LANES:] = low
        keys = kh_ref[slot0 + i]
        values = vh_ref[slot0 + i]
        for start in range(0, tokens, tile):
            end = start + tile
            scores = lax.dot_general(queries[start:end], keys[:end], (((1,), (1,)), ((), ())), preferred_element_type=F32)
            gaps = cols[start:end, i : i + 1] - cum[i : i + 1, :end]
            inside = jnp.where(causal, gaps[:, start:], -jnp.inf)
            if start:
                gaps = jnp.concatenate([gaps[:, :start], inside], axis=1)
            else:
                gaps = inside
            masked = (scores * jnp.exp(gaps)).astype(BF16)
            intra_ref[i, start:end] = jnp.dot(masked, values[:end], preferred_element_type=F32)


def inside_block(group, slot0, log_decay, query_rows, kh, vh):
    tokens, _, width = query_rows.shape
    return pl.pallas_call(
        functools.partial(inside_kernel, 128, group * SUB, slot0),
        in_specs=[VM] * 4,
        out_specs=[VM] * 2,
        out_shape=[
            jax.ShapeDtypeStruct((SUB, tokens, width), F32),
            jax.ShapeDtypeStruct((SUB, tokens, 2 * width), BF16),
        ],
        scratch_shapes=[pltpu.VMEM((tokens * SUB, width), F32)],
        cost_estimate=pl.CostEstimate(flops=4 * SUB * tokens * tokens * width, transcendentals=SUB * tokens * tokens, bytes_accessed=12 * SUB * tokens * width),
        compiler_params=pltpu.CompilerParams(vmem_limit_bytes=LIMITS["inside"] * MIB),
        name="inside",
    )(log_decay, query_rows, kh, vh)


def output_kernel(tiled, head0, groups, *refs):
    intra, q2 = refs[:groups], refs[groups : 2 * groups]
    if tiled:
        near_ref, far_ref = refs[2 * groups : 2 * groups + 2]
        core, xbit = position()
        at = 2 * groups + 2
    else:
        state_ref = refs[2 * groups]
        at = 2 * groups + 1
    if head0:
        at += 1
    out_ref, flat, packed, sems = refs[at:]
    tokens = out_ref.shape[0]
    copies = []
    for g in range(groups):
        for i in range(SUB):
            slot = g * SUB + i
            if tiled:
                pieces = []
                for z in range(near_ref.shape[1]):
                    for x in range(2):
                        for c in range(2):
                            a = near_ref if c == 0 else far_ref
                            b = far_ref if c == 0 else near_ref
                            plain = jnp.where(core, b[x, z, slot], a[x, z, slot])
                            flipped = jnp.where(core, b[1 - x, z, slot], a[1 - x, z, slot])
                            pieces.append(jnp.where(xbit, flipped, plain))
                carried = jnp.concatenate(pieces, axis=0)
            else:
                carried = state_ref[slot]
            hi, low = split2(carried)
            right = jnp.concatenate([jnp.concatenate([hi, low], axis=1), jnp.concatenate([hi, jnp.zeros_like(low)], axis=1)], axis=0)
            both = jnp.dot(q2[g][i], right, preferred_element_type=F32)
            mixed = intra[g][i] + (both[:, :LANES] + both[:, LANES:])
            mean = jnp.mean(mixed * mixed, axis=1, keepdims=True)
            flat[pl.ds(i, tokens, stride=SUB), :] = mixed * lax.rsqrt(mean + norm_eps)
        packed[g] = flat[...].reshape(tokens, SUB, LANES).astype(BF16)
        copies.append(pltpu.make_async_copy(packed.at[g], out_ref.at[:, pl.ds(head0 + g * SUB, SUB), :], sems.at[g]))
        copies[-1].start()
    for copy in copies:
        copy.wait()


def outputs(tiled, heads, head0, insides, attended, *carried):
    groups = len(insides)
    intra, q2 = zip(*insides)
    _, tokens, width = intra[0].shape
    args = intra + q2 + carried
    specs = [VM] * len(args)
    alias = {}
    if head0:
        args += (attended,)
        specs.append(HBM)
        alias = {len(args) - 1: 0}
    return pl.pallas_call(
        functools.partial(output_kernel, tiled, head0, groups),
        in_specs=specs,
        out_specs=HBM,
        out_shape=jax.ShapeDtypeStruct((tokens, heads, width), BF16),
        scratch_shapes=[
            pltpu.VMEM((tokens * SUB, width), F32),
            pltpu.VMEM((groups, tokens, SUB, width), BF16),
            pltpu.SemaphoreType.DMA((groups,)),
        ],
        input_output_aliases=alias,
        cost_estimate=pl.CostEstimate(flops=4 * groups * SUB * tokens * width * width, transcendentals=2 * groups * SUB * tokens, bytes_accessed=8 * groups * SUB * tokens * width),
        compiler_params=pltpu.CompilerParams(vmem_limit_bytes=LIMITS["outputs"] * MIB),
        name="outputs",
    )(*args)


def decode_kernel(chunks, n, q_ref, k_ref, v_ref, d_ref, state_hbm, end_ref, near_ref, before_ref, qf, kf, vf, sbuf, sf, sems):
    steps, heads, width = q_ref.shape
    me = lax.axis_index("seq")
    block = lax.div(me, SUB)
    copies = []
    for c in range(chunks):
        start = pl.multiple_of(c * n + block * SUB, SUB)
        copies.append(pltpu.make_async_copy(state_hbm.at[:, pl.ds(start, SUB), :], sbuf.at[c], sems.at[c]))
        copies[-1].start()
    flatten(q_ref[...], qf)
    flatten(k_ref[...], kf)
    flatten(v_ref[...], vf)
    t = lax.broadcasted_iota(jnp.int32, (steps, LANES), 0)
    s = lax.broadcasted_iota(jnp.int32, (steps, LANES), 1)
    for c in range(chunks):
        head = c * n + me
        q, k, v = (f[pl.ds(head, steps, stride=heads), :] for f in (qf, kf, vf))
        lane = lax.broadcasted_iota(jnp.int32, (steps, heads), 1)
        own = jnp.sum(jnp.where(lane == head, d_ref[...], 0.0), axis=1, keepdims=True)
        order = lax.broadcasted_iota(jnp.int32, (steps, 1), 0)
        cum = jnp.zeros((steps, 1), F32)
        for u in range(steps):
            cum = cum + jnp.where(order >= u, own[u : u + 1], 0.0)
        column = jnp.broadcast_to(cum, (steps, LANES))
        row = jnp.sum(jnp.where(t == s, column, 0.0), axis=0, keepdims=True)
        pair = jnp.exp(jnp.where((t >= s) & (s < steps), column - row, -jnp.inf))
        end_ref[c] = jnp.exp(column)
        scores = lax.dot_general(q.astype(BF16), k.astype(BF16), (((1,), (1,)), ((), ())), preferred_element_type=F32)
        near = jnp.zeros((steps, width), F32)
        for u in range(steps):
            near = near + (scores[:, u : u + 1] * pair[:, u : u + 1]) * v[u : u + 1]
        near_ref[c] = near
        copies[c].wait()
        sf[...] = sbuf[c].reshape(width * SUB, width)
        state = sf[pl.ds(lax.rem(me, SUB), width, stride=SUB), :]
        before = None
        for piece in split3(state):
            part = jnp.dot(q.astype(BF16), piece, preferred_element_type=F32)
            before = part if before is None else before + part
        before_ref[c] = before


def decode_terms(chunks, n, decode_query, decode_key, decode_value, decode_decay, state_in):
    steps, heads, width = decode_query.shape
    out = jax.ShapeDtypeStruct((chunks, steps, width), F32)
    return pl.pallas_call(
        functools.partial(decode_kernel, chunks, n),
        in_specs=[VM] * 4 + [HBM],
        out_specs=[VM] * 3,
        out_shape=[out] * 3,
        scratch_shapes=[pltpu.VMEM((steps * heads, width), F32)] * 3
        + [
            pltpu.VMEM((chunks, width, SUB, width), F32),
            pltpu.VMEM((width * SUB, width), F32),
            pltpu.SemaphoreType.DMA((chunks,)),
        ],
        cost_estimate=pl.CostEstimate(flops=1 << 20, transcendentals=1 << 10, bytes_accessed=MIB),
        compiler_params=pltpu.CompilerParams(vmem_limit_bytes=LIMITS["decode"] * MIB),
        name="decode",
    )(decode_query, decode_key, decode_value, decode_decay, state_in)


def normalize(mixed):
    return mixed * lax.rsqrt(jnp.mean(mixed * mixed, axis=-1, keepdims=True) + norm_eps)


LIMITS = {"states": 24, "inside": 12, "outputs": 12, "decode": 4}


def local(query_rows, key_rows, value_rows, log_decay, state_in, decode_query, decode_key, decode_value, decode_decay):
    tokens, heads, width = query_rows.shape
    steps = decode_query.shape[0]
    n = lax.axis_size("seq")
    me = lax.axis_index("seq")
    spans = n // 4
    rows = width // n
    core, xbit, z = me % 2, (me // 2) % 2, me // 4
    tiled = rows % SUB == 0
    pseudo = tiled and rows == steps and heads % n == 0 and n % SUB == 0 and n * steps == width
    chunks = heads // n if pseudo else 1
    per = heads // chunks
    slots = per + (1 if pseudo else 0)

    swap_core = [(i, i ^ 1) for i in range(n)]
    swap_x = [(i, i ^ 2) for i in range(n)]
    shift = lambda s: [(i, (i + 4 * s) % n) for i in range(n)]

    def first(flag, a, b):
        return jnp.where(flag == 0, a, b)

    def weights(total, part):
        w = jnp.exp(total)[:, None, :]
        if pseudo:
            lead = part.shape[:-1]
            w = jnp.broadcast_to(w, lead + w.shape)
            w = jnp.concatenate([w, jnp.exp(part)[..., None, None, :]], axis=len(lead))
        return w

    def owners(total, x_rel):
        if not pseudo:
            return None
        t = total.reshape(spans, 2, 2, LANES)
        t = lax.dynamic_index_in_dim(t, core, 2, keepdims=False)
        return lax.dynamic_index_in_dim(t, (xbit + x_rel) % 2, 1, keepdims=False)

    def swap(flat, shape, count, pairs):
        got = lax.ppermute(flat, "seq", pairs)
        return got[:-count].reshape(shape), got[-count:]

    def exchange(x, total, pairs):
        flat = jnp.concatenate([x.reshape(-1, width), total], axis=0)
        return swap(flat, x.shape, total.shape[0], pairs)

    def to_absolute(pieces):
        turned = jnp.stack(pieces[::-1] + pieces[:0:-1])
        return lax.dynamic_slice_in_dim(turned, spans - 1 - z, spans, 0)

    kept, by_head = [], []
    left = None
    for c in range(chunks):
        if c == 0:
            made = states(c, per, tiled, pseudo, rows, spans, (log_decay, decode_query, key_rows, value_rows))
            left = made[5:]
        else:
            made = states(c, per, tiled, pseudo, rows, spans, (left[0], left[1], decode_query, left[2], left[3]))
        keep, send, total, kh, vh = made[:5]
        if not tiled:
            parts = jnp.transpose(keep.reshape(per, spans, 2, 2, rows, width), (3, 2, 1, 0, 4, 5))
            parts = jnp.where(xbit == 0, parts, parts[:, ::-1])
            keep, send = first(core, parts[0], parts[1]), first(core, parts[1], parts[0])
            send = jnp.concatenate([send.reshape(-1, width), total], axis=0)
        kept.append((keep, send, total))
        by_head.append((kh, vh))

    groups = per // SUB
    insides = [
        [inside_block(c * groups + g, g * SUB, log_decay, query_rows, *by_head[c]) for g in range(groups)]
        for c in range(chunks)
    ]
    if pseudo:
        from_end, near, before = decode_terms(chunks, n, decode_query, decode_key, decode_value, decode_decay, state_in)
    prior = jnp.transpose(lax.dynamic_slice_in_dim(state_in, me * rows, rows, 0), (1, 0, 2))

    level = []
    for c in range(chunks):
        keep, send, total = kept[c]
        got, got_total = swap(send, keep.shape, per, swap_core)
        part = lambda t: jnp.stack([owners(t, 0), owners(t, 1)]) if pseudo else None
        mine = first(core, weights(got_total, part(got_total)), 1.0)
        theirs = first(core, 1.0, weights(total, part(total)))
        chip = keep * mine + got * theirs
        chip_total = total + got_total
        got_x, got_x_total = exchange(chip[1], chip_total, swap_x)
        mine = first(xbit, weights(got_x_total, owners(got_x_total, 0)), 1.0)
        theirs = first(xbit, 1.0, weights(chip_total, owners(chip_total, 0)))
        span = chip[0] * mine + got_x * theirs
        level.append((got, got_total, chip, chip_total, got_x, got_x_total, span, chip_total + got_x_total))

    finals, carries = [], []
    for c in range(chunks):
        span, span_total = level[c][6:]
        pieces = [lax.dynamic_index_in_dim(span, z, 0, keepdims=False)]
        totals = [span_total]
        for s in range(1, spans):
            piece, t = exchange(lax.dynamic_index_in_dim(span, (z + s) % spans, 0, keepdims=False), span_total, shift(s))
            pieces.append(piece)
            totals.append(t)
        pieces, totals = to_absolute(pieces), to_absolute(totals)
        carried = prior[c * per : (c + 1) * per]
        if pseudo:
            carried = jnp.concatenate([carried, before[c][None]], axis=0)
        all_carried = []
        for s in range(spans):
            all_carried.append(carried)
            t = totals[s]
            own = lax.dynamic_index_in_dim(t, me, 0, keepdims=False) if pseudo else None
            carried = carried * weights(t, own) + pieces[s]
        finals.append(carried[:per])
        if pseudo:
            dec = normalize(carried[per] * from_end[c] + near[c])
            all_carried = [jnp.concatenate([a[:per], dec[None]], axis=0) for a in all_carried]
        all_carried = jnp.stack(all_carried)
        pieces = [lax.dynamic_index_in_dim(all_carried, z, 0, keepdims=False)]
        for s in range(1, spans):
            pieces.append(lax.ppermute(lax.dynamic_index_in_dim(all_carried, (z + s) % spans, 0, keepdims=False), "seq", shift(s)))
        carries.append(to_absolute(pieces))

    slot = lax.broadcasted_iota(jnp.int32, (slots, 1, 1), 0)

    def advance(carried, total, state):
        w = jnp.exp(total)[:, None, :]
        if not pseudo:
            return carried * w + state
        w = jnp.concatenate([w, jnp.ones((1, 1, LANES), F32)], axis=0)
        return carried * w + jnp.where(slot < per, state, 0.0)

    attended, dec_out = None, []
    for c in range(chunks):
        keep, send, total = kept[c]
        got, got_total, chip, chip_total, got_x, got_x_total, _, _ = level[c]
        at_span = carries[c]
        msg = first(xbit, advance(at_span, chip_total, chip[0]), at_span)
        own = first(xbit, at_span, advance(at_span, got_x_total, got_x))
        at_chip = jnp.stack([own, lax.ppermute(msg, "seq", swap_x)])
        msg = first(core, advance(at_chip, total, keep), at_chip)
        own = first(core, at_chip, advance(at_chip, got_total, got))
        other = lax.ppermute(msg, "seq", swap_core)
        if tiled:
            carried = (own, other)
        else:
            both = jnp.stack([first(core, own, other), first(core, other, own)])
            both = jnp.where(xbit == 0, both, both[:, ::-1])
            carried = (jnp.transpose(both, (3, 2, 1, 0, 4, 5)).reshape(per, width, width),)
        attended = outputs(tiled, heads, c * per, insides[c], attended, *carried)
        if pseudo:
            both = jnp.stack([first(core, own[:, :, per], other[:, :, per]), first(core, other[:, :, per], own[:, :, per])])
            both = jnp.where(xbit == 0, both, both[:, ::-1])
            dec_out.append(jnp.transpose(both, (3, 2, 1, 0, 4)).reshape(steps, per, width))

    final_rows = jnp.transpose(jnp.concatenate(finals, axis=0), (1, 0, 2))
    if pseudo:
        decode_out = jnp.concatenate(dec_out, axis=1)
    else:
        start = me * rows
        key_part = lax.dynamic_slice_in_dim(decode_key, start, rows, 2).astype(F32)
        query_part = lax.dynamic_slice_in_dim(decode_query, start, rows, 2).astype(F32)
        order = jnp.arange(steps)
        causal = order[:, None, None] >= order[None, :, None]
        cum = jnp.cumsum(decode_decay, axis=0)
        pair = jnp.exp(jnp.where(causal, cum[:, None] - cum[None, :], -jnp.inf))
        scores = jnp.einsum("thr,shr->tsh", query_part, key_part, precision=HIGH) * pair
        inside = jnp.einsum("tsh,she->the", scores, decode_value.astype(F32), precision=HIGH)
        far = jnp.einsum("thr,rhe->the", query_part, final_rows, precision=HIGH) * jnp.exp(cum)[:, :, None]
        decode_out = normalize(lax.psum(inside + far, "seq"))
    return attended, final_rows, decode_out


def solution(mesh):
    in_specs = (
        P("seq", "head", None),
        P("seq", "head", None),
        P("seq", "head", None),
        P("seq", "head"),
        P(None, "head", None),
        P(None, "head", None),
        P(None, "head", None),
        P(None, "head", None),
        P(None, "head"),
    )
    out_specs = (P("seq", "head", None), P("seq", "head", None), P(None, "head", None))
    return jax.shard_map(local, mesh=mesh, in_specs=in_specs, out_specs=out_specs, check_vma=False)
```
